128 devices in a mesh: row: 16 (over y, z), col: 8 (over x, core).
Axes of the slice: x: 4, y: 4, z: 4, core: 2. Of those that a mesh axis runs over, the one named last changes fastest.
Arguments:
- grid_values: bfloat16 [512, 256, 384], P(('row', 'col')), may hold values from -0.109375 to 0.109375
- external: float32 [512, 256], P(('row', 'col')), may hold values from 0 to 6
- tiles: int32 [512, 3], P(('row', 'col')), may hold values from 0 to 15, as said below
- kinetic: bfloat16 [16384, 16384], P('row', 'col'), may hold values from -0.046875 to 0.046875
- orbitals: bfloat16 [16384, 256], P(('row', 'col')), may hold values from -6 to 6
Outputs:
- filtered: float32 [16384, 256], P(('row', 'col'))
The draws below stay inside these ranges and needn't reach their ends.
Inputs may be any that keep to these rules, and one draw needn't show every extreme that they name: Each batch names 3 distinct tiles in increasing order. Among the 4 batches of one device no tile is named more than 2 times; in every draw some tile is named exactly 2 times by the batches of every device.
All inputs are finite; a program needn't handle non-finite values.
Results may differ from the reference program's by a relative error of at most 0.0064.
Values may be sent and summed in bfloat16 or wider, within the bound.
A program may use at most 128 MiB of HBM per device.

```python
import jax
import jax.numpy as jnp
from jax import lax

NB = 16384
NORB = 256
TILE = 128
LISTED = 3
CAP = 2
B_DEV = 4
PTS = 256
LIST = 384
BATCHES = 512
TPC = 16
TILE_HITS = 12
N_ROW = 16
N_COL = 8
DEVICES = 128


def draw_tiles(key, part):
    tickets = TPC * CAP
    favored = jax.random.randint(jax.random.fold_in(key, 7), (), 0, TPC)

    def one_device(device_key):
        drawn = jax.random.randint(device_key, (tickets,), 0, tickets)
        ticket_ids = jnp.arange(tickets, dtype=jnp.int32)
        scores = drawn * tickets + ticket_ids
        scores = jnp.where(ticket_ids // CAP == favored, tickets * tickets + ticket_ids, scores)
        _, chosen = lax.top_k(scores, B_DEV * LISTED)
        chosen = jnp.sort(chosen)
        return (chosen // CAP).reshape(LISTED, B_DEV).T
    device_keys = jax.random.split(jax.random.fold_in(key, 11), DEVICES)
    return jax.vmap(one_device)(device_keys).reshape(DEVICES * B_DEV, LISTED).astype(jnp.int32)


def level_of(stream_key, shape, shards, least, largest):
    factor_of = 1.0
    for position, parts in shards:
        heights = jax.random.uniform(jax.random.fold_in(jax.random.fold_in(stream_key, 6), position), (parts,), jnp.float32, least / len(shards), largest / len(shards))
        factor_of = factor_of * jnp.repeat(jnp.exp(heights), shape[position] // parts).reshape((-1,) + (1,) * (len(shape) - 1 - position))
    return factor_of


def gaussian(rng, dims, deviation, bound, shards=(), held_as=jnp.bfloat16):
    array = jax.random.normal(rng, dims, jnp.float32) * deviation
    if len(shards) > 0:
        array = level_of(rng, dims, shards, -0.22, 0.18) * array
    return jnp.clip(array, min=-bound, max=bound).astype(held_as)


def setup_inputs(seed: int = 0) -> dict:
    key_list = jax.random.split(jax.random.key(seed), 6)
    grid_values = gaussian(key_list[0], (BATCHES, PTS, LIST), (PTS * TILE_HITS) ** -0.5, 0.109375, ((0, 128),))
    external = jnp.clip(6.0 * jax.random.uniform(key_list[1], (BATCHES, PTS), jnp.float32) ** level_of(key_list[1], (BATCHES, PTS), ((0, 128),), -0.2, 0.2), 0.0, 6.0)
    tiles = draw_tiles(jax.random.fold_in(key_list[5], 71), 0)
    kinetic = gaussian(key_list[3], (NB, NB), NB ** -0.5, 0.046875, ((0, 16), (1, 8)))
    orbitals = gaussian(key_list[4], (NB, NORB), 1.0, 6.0, ((0, 128),))
    return dict(grid_values=grid_values, external=external, tiles=tiles, kinetic=kinetic, orbitals=orbitals)


center = 1.0
spread = 2.5


def reference(grid_values, external, tiles, kinetic, orbitals):
    shard_rows = NB // (N_ROW * N_COL)
    per_shard = shard_rows // TILE
    column_group = (jnp.arange(BATCHES, dtype=jnp.int32) // B_DEV) % N_COL
    starts = ((tiles // per_shard) * N_COL + column_group[:, None]) * shard_rows + (tiles % per_shard) * TILE
    listed = (starts[:, :, None] + jnp.arange(TILE, dtype=jnp.int32)[None, None, :]).reshape(BATCHES, LIST).astype(jnp.int32)

    def one_batch(summed_grid, inputs):
        values, outside, index = inputs
        waves = jnp.dot(values, orbitals[index], preferred_element_type=jnp.float32)
        density = jnp.sum(waves * waves, axis=1)
        potential = outside - jnp.cbrt(3.0 * density / jnp.pi)
        weighted = (potential[:, None] * values.astype(jnp.float32)).astype(jnp.bfloat16)
        integral = jnp.dot(values.T, weighted, preferred_element_type=jnp.float32)
        summed_grid = summed_grid.at[index[:, None], index[None, :]].add(integral)
        return summed_grid, None

    grid_matrix, _ = lax.scan(one_batch, jnp.zeros((NB, NB), jnp.float32), (grid_values, external, listed))
    ordered = kinetic.reshape(NB, N_COL, N_ROW, shard_rows).transpose(0, 2, 1, 3).reshape(NB, NB)
    hamiltonian = (ordered.astype(jnp.float32) + grid_matrix).astype(jnp.bfloat16)

    def apply(vectors):
        return jnp.dot(hamiltonian, vectors, preferred_element_type=jnp.float32) / spread - (center / spread) * vectors.astype(jnp.float32)

    filtered_one = apply(orbitals).astype(jnp.bfloat16)
    filtered_two = (2.0 * apply(filtered_one) - orbitals.astype(jnp.float32)).astype(jnp.bfloat16)
    return 2.0 * apply(filtered_two) - filtered_one.astype(jnp.float32)
```

```python
import jax
import jax.numpy as jnp
from jax import lax
from jax.experimental import pallas as pl
from jax.experimental.pallas import tpu as pltpu
from jax.sharding import PartitionSpec as P

MESH = pl.DeviceIdType.MESH
TILE = 128
NORB = 256
LISTED = 3
BATCH = 4
PTS = 256
LIST = 384
SLOTS = BATCH * LISTED
HALF = TILE // 2
FAR = (2, 1, 3)
NEAR = (1, 3, 2)
BF = jnp.bfloat16
F32 = jnp.float32
center = 1.0
spread = 2.5


def kernel(
    tiles_ref, ext_ref, g_hbm, k_hbm, orb_hbm, out_ref,
    kin, g, gt, v, sb, r1, r2, cb, cr, pot, yb, inv,
    load_sem, ag_s, ag_r, r1_s, r1_r, r2_s, r2_r, c_s, c_r,
):
    row, col = lax.axis_index("row"), lax.axis_index("col")
    y, z = row // 4, row % 4
    x, core = col // 2, col % 2

    def at(dy, dz):
        return lax.rem(y + dy, 4) * 4 + lax.rem(z + dz, 4)

    def tile_of(h, p, q):
        return at(q, p) if h == 0 else at(p, q)

    load_k = pltpu.make_async_copy(k_hbm, kin, load_sem.at[0])
    load_g = pltpu.make_async_copy(g_hbm, g, load_sem.at[1])
    load_v = pltpu.make_async_copy(orb_hbm, v.at[0, row], load_sem.at[2])
    load_v.start()
    load_g.start()
    load_k.start()

    barrier = pltpu.get_barrier_semaphore()
    peers = [(at(0, d), col) for d in NEAR] + [(at(d, 0), col) for d in NEAR]
    peers += [(row, lax.rem(col + d, 8)) for d in range(1, 8)]
    for peer in peers:
        pl.semaphore_signal(barrier, inc=1, device_id=peer, device_id_type=MESH)

    def invert(u, carry):
        first, second = jnp.int32(SLOTS), jnp.int32(SLOTS)
        for s in range(SLOTS):
            hit = tiles_ref[s // LISTED, s % LISTED] == u
            second = jnp.where(hit & (first < SLOTS), s, second)
            first = jnp.where(hit & (first == SLOTS), s, first)
        inv[0, u] = first
        inv[1, u] = second
        return carry

    lax.fori_loop(0, 16, invert, 0)
    yb[SLOTS] = jnp.zeros((TILE, NORB), F32)
    pl.semaphore_wait(barrier, len(peers))
    load_v.wait()

    def gather(k):
        sends = []

        def send(h, p, q, dp, dq):
            part = v.at[k, tile_of(h, p, q), pl.ds(h * HALF, HALF)]
            rp, rq = (p - dp) % 4, (q - dq) % 4
            copy = pltpu.make_async_remote_copy(
                src_ref=part,
                dst_ref=part,
                send_sem=ag_s.at[h, rp, rq],
                recv_sem=ag_r.at[k, h, rp, rq],
                device_id=(tile_of(h, dp, dq), col),
                device_id_type=MESH,
            )
            copy.start()
            sends.append(copy)

        def arrive(h, p, q):
            part = v.at[k, tile_of(h, p, q), pl.ds(h * HALF, HALF)]
            pltpu.make_async_remote_copy(
                src_ref=part, dst_ref=part, send_sem=ag_s.at[h, p, q], recv_sem=ag_r.at[k, h, p, q],
                device_id=(row, col), device_id_type=MESH,
            ).wait_recv()

        for d in NEAR:
            for h in range(2):
                send(h, 0, 0, d, 0)
        for d in NEAR:
            for h in range(2):
                send(h, 0, 0, 0, d)
        for p in NEAR:
            for h in range(2):
                arrive(h, p, 0)
                for d in NEAR:
                    send(h, p, 0, 0, d)
        return sends, arrive

    def arrive_all(arrive):
        for p in (0, *NEAR):
            for q in NEAR:
                for h in range(2):
                    arrive(h, p, q)

    def waves_of(k, b):
        listed = jnp.concatenate([v[k, tiles_ref[b, s]] for s in range(LISTED)], axis=0)
        return jnp.dot(g[b], listed, preferred_element_type=F32)

    def scatter(k):
        sends, built = [], set()

        def build(dy, dz):
            if (dy, dz) in built:
                return
            built.add((dy, dz))
            u = at(dy, dz)
            sb[k, u] = (yb[inv[0, u]] + yb[inv[1, u]]).astype(BF)

        for q in (*FAR, 0):
            for d in FAR:
                build(q, d)
                build(d, q)
                for h in range(2):
                    rp = (-d) % 4
                    copy = pltpu.make_async_remote_copy(
                        src_ref=sb.at[k, tile_of(h, d, q), pl.ds(h * HALF, HALF)],
                        dst_ref=r1.at[k, h, q, rp],
                        send_sem=r1_s.at[h, q, rp],
                        recv_sem=r1_r.at[k, h, q, rp],
                        device_id=(tile_of(h, d, 0), col),
                        device_id_type=MESH,
                    )
                    copy.start()
                    sends.append(copy)
        build(0, 0)
        return sends

    def kinetic(k):
        sends = []
        vectors = v[k].reshape(16 * TILE, NORB)
        for dx in (*FAR, 0):
            there = lax.rem(x + dx, 4)
            rows = pl.ds(pl.multiple_of(there * 256, 256), 256)
            part = jnp.dot(kin[rows, :], vectors, preferred_element_type=F32)
            cb[k, there] = part.astype(BF).reshape(2, TILE, NORB)
            if dx == 0:
                targets = [1 - core]
            else:
                targets = [0, 1]
            for n, e in enumerate(targets):
                rx = (-dx) % 4
                copy = pltpu.make_async_remote_copy(
                    src_ref=cb.at[k, there, e],
                    dst_ref=cr.at[k, rx, core],
                    send_sem=c_s.at[dx, n],
                    recv_sem=c_r.at[k, rx, core],
                    device_id=(row, there * 2 + e),
                    device_id_type=MESH,
                )
                copy.start()
                sends.append(copy)
        return sends

    def pass_on(k):
        sends, kept = [], []
        for q in (*FAR, 0):
            for h in range(2):
                total = sb[k, tile_of(h, 0, q), pl.ds(h * HALF, HALF)].astype(F32)
                for p in FAR:
                    pltpu.make_async_remote_copy(
                        src_ref=r1.at[k, h, q, p], dst_ref=r1.at[k, h, q, p], send_sem=r1_s.at[h, q, p],
                        recv_sem=r1_r.at[k, h, q, p], device_id=(row, col), device_id_type=MESH,
                    ).wait_recv()
                    total = total + r1[k, h, q, p].astype(F32)
                if q == 0:
                    kept.append(total)
                    continue
                own = sb.at[k, tile_of(h, 0, q), pl.ds(h * HALF, HALF)]
                own[...] = total.astype(BF)
                rq = (-q) % 4
                copy = pltpu.make_async_remote_copy(
                    src_ref=own,
                    dst_ref=r2.at[k, h, rq],
                    send_sem=r2_s.at[h, rq],
                    recv_sem=r2_r.at[k, h, rq],
                    device_id=(tile_of(h, 0, q), col),
                    device_id_type=MESH,
                )
                copy.start()
                sends.append(copy)
        return sends, kept

    def collect(k, kept):
        total = cb[k, x, core].astype(F32)
        for dx in (0, *NEAR):
            for e in [1 - core] if dx == 0 else [0, 1]:
                pltpu.make_async_remote_copy(
                    src_ref=cr.at[k, dx, e], dst_ref=cr.at[k, dx, e], send_sem=c_s.at[0, 0],
                    recv_sem=c_r.at[k, dx, e], device_id=(row, col), device_id_type=MESH,
                ).wait_recv()
                total = total + cr[k, dx, e].astype(F32)
        halves = []
        for h in range(2):
            part = kept[h]
            for q in NEAR:
                pltpu.make_async_remote_copy(
                    src_ref=r2.at[k, h, q], dst_ref=r2.at[k, h, q], send_sem=r2_s.at[h, q],
                    recv_sem=r2_r.at[k, h, q], device_id=(row, col), device_id_type=MESH,
                ).wait_recv()
                part = part + r2[k, h, q].astype(F32)
            halves.append(part)
        return total + jnp.concatenate(halves, axis=0)

    for k in range(3):
        sends, arrive = gather(k)
        if k == 0:
            load_g.wait()
            for b in range(BATCH):
                gt[b] = g[b].T
            ext = ext_ref[...]
            ext = jnp.concatenate([ext, ext], axis=0).T
        arrive_all(arrive)
        for b in range(BATCH):
            waves = waves_of(k, b)
            if k == 0:
                density = jnp.sum(waves * waves, axis=1, keepdims=True)
                root = jnp.exp(jnp.log(density * (3.0 / jnp.pi)) * (1.0 / 3.0))
                pot[b] = jnp.broadcast_to(ext[:, b : b + 1] - root, (PTS, NORB))
            term = (pot[b] * waves).astype(BF)
            yb[pl.ds(b * LISTED, LISTED)] = jnp.dot(gt[b], term, preferred_element_type=F32).reshape(
                LISTED, TILE, NORB
            )
        sends += scatter(k)
        if k == 0:
            load_k.wait()
        sends += kinetic(k)
        more, kept = pass_on(k)
        sends += more
        product = collect(k, kept)
        own = v[k, row].astype(F32)
        applied = product / spread - (center / spread) * own
        if k == 0:
            v[1, row] = applied.astype(BF)
        else:
            result = 2.0 * applied - v[k - 1, row].astype(F32)
            if k == 1:
                v[2, row] = result.astype(BF)
            else:
                out_ref[...] = result
        for copy in sends:
            copy.wait_send()


def body(grid_values, external, tiles, kinetic, orbitals):
    any_spec = pl.BlockSpec(memory_space=pl.ANY)
    dma = pltpu.SemaphoreType.DMA
    return pl.pallas_call(
        kernel,
        out_shape=jax.ShapeDtypeStruct((TILE, NORB), F32),
        in_specs=[
            pl.BlockSpec(memory_space=pltpu.SMEM),
            pl.BlockSpec(memory_space=pltpu.VMEM),
            any_spec,
            any_spec,
            any_spec,
        ],
        out_specs=pl.BlockSpec(memory_space=pltpu.VMEM),
        scratch_shapes=[
            pltpu.VMEM(kinetic.shape, BF),
            pltpu.VMEM((BATCH, PTS, LIST), BF),
            pltpu.VMEM((BATCH, LIST, PTS), BF),
            pltpu.VMEM((3, 16, TILE, NORB), BF),
            pltpu.VMEM((3, 16, TILE, NORB), BF),
            pltpu.VMEM((3, 2, 4, 4, HALF, NORB), BF),
            pltpu.VMEM((3, 2, 4, HALF, NORB), BF),
            pltpu.VMEM((3, 4, 2, TILE, NORB), BF),
            pltpu.VMEM((3, 4, 2, TILE, NORB), BF),
            pltpu.VMEM((BATCH, PTS, NORB), F32),
            pltpu.VMEM((SLOTS + 1, TILE, NORB), F32),
            pltpu.SMEM((2, 16), jnp.int32),
            dma((3,)),
            dma((2, 4, 4)),
            dma((3, 2, 4, 4)),
            dma((2, 4, 4)),
            dma((3, 2, 4, 4)),
            dma((2, 4)),
            dma((3, 2, 4)),
            dma((4, 2)),
            dma((3, 4, 2)),
        ],
        compiler_params=pltpu.CompilerParams(
            collective_id=0, has_side_effects=True, vmem_limit_bytes=60 * 1024 * 1024
        ),
    )(tiles, external, grid_values, kinetic, orbitals)


def solution(mesh):
    return jax.shard_map(
        body,
        mesh=mesh,
        in_specs=(
            P(("row", "col"), None, None),
            P(("row", "col"), None),
            P(("row", "col"), None),
            P("row", "col"),
            P(("row", "col"), None),
        ),
        out_specs=P(("row", "col"), None),
        check_vma=False,
    )
```

```python
import jax
import jax.numpy as jnp
from jax import lax
from jax.experimental import pallas as pl
from jax.experimental.pallas import tpu as pltpu
from jax.sharding import PartitionSpec as P

MESH = pl.DeviceIdType.MESH
TILE = 128
STREAMS = 2
LANES = 128
LISTED = 3
BATCH = 4
PTS = 256
LIST = 384
SLOTS = BATCH * LISTED
HALF = TILE // 2
FAR = (2, 1, 3)
NEAR = (1, 3, 2)
BF = jnp.bfloat16
F32 = jnp.float32
center = 1.0
spread = 2.5


def kernel(
    tiles_ref, ext_ref, g_hbm, k_hbm, orb_hbm, out_ref,
    kin, g, gt, v_one, v_two, sb, r1, r2, cb, cr, pot, yb, inv,
    load_sem, near_r, far_r, rest_r, r1_r, r2_r, c_r, ag_s, r1_s, r2_s, c_s,
):
    v = (v_one, v_two)
    row, col = lax.axis_index("row"), lax.axis_index("col")
    y, z = row // 4, row % 4
    x, core = col // 2, col % 2

    def at(dy, dz):
        return lax.rem(y + dy, 4) * 4 + lax.rem(z + dz, 4)

    def tile_of(h, p, q):
        return at(q, p) if h == 0 else at(p, q)

    def start(src, dst, send, recv, target):
        pltpu.make_async_remote_copy(
            src_ref=src, dst_ref=dst, send_sem=send, recv_sem=recv, device_id=target, device_id_type=MESH
        ).start()

    def arrived(ref, recv):
        pltpu.make_async_remote_copy(
            src_ref=ref, dst_ref=ref, send_sem=recv, recv_sem=recv, device_id=(row, col), device_id_type=MESH
        ).wait_recv()

    def sent(ref, send):
        pltpu.make_async_remote_copy(
            src_ref=ref, dst_ref=ref, send_sem=send, recv_sem=send, device_id=(row, col), device_id_type=MESH
        ).wait_send()

    load_k = pltpu.make_async_copy(k_hbm, kin, load_sem.at[0])
    load_g = pltpu.make_async_copy(g_hbm, g, load_sem.at[1])
    load_v = [
        pltpu.make_async_copy(orb_hbm.at[:, pl.ds(s * LANES, LANES)], v[s].at[0, row], load_sem.at[2 + s])
        for s in range(STREAMS)
    ]
    for load in load_v:
        load.start()
    load_g.start()
    load_k.start()

    barrier = pltpu.get_barrier_semaphore()
    peers = [(at(0, d), col) for d in NEAR] + [(at(d, 0), col) for d in NEAR]
    peers += [(row, lax.rem(col + d, 8)) for d in range(1, 8)]
    for peer in peers:
        pl.semaphore_signal(barrier, inc=1, device_id=peer, device_id_type=MESH)

    def invert(u, carry):
        first, second = jnp.int32(SLOTS), jnp.int32(SLOTS)
        for n in range(SLOTS):
            hit = tiles_ref[n // LISTED, n % LISTED] == u
            second = jnp.where(hit & (first < SLOTS), n, second)
            first = jnp.where(hit & (first == SLOTS), n, first)
        inv[0, u] = first
        inv[1, u] = second
        return carry

    lax.fori_loop(0, 16, invert, 0)
    for s in range(STREAMS):
        yb[s, SLOTS] = jnp.zeros((TILE, LANES), F32)
    pl.semaphore_wait(barrier, len(peers))
    for load in load_v:
        load.wait()

    def pass_tile(k, s, h, p, q, dp, dq):
        part = v[s].at[k, tile_of(h, p, q), pl.ds(h * HALF, HALF)]
        if dq:
            recv = rest_r.at[k, s]
        else:
            recv = far_r.at[k, s] if dp == 2 else near_r.at[k, s]
        start(part, part, ag_s.at[s], recv, (tile_of(h, dp, dq), col))

    def gather_own(k, s):
        for d in NEAR:
            for h in range(2):
                pass_tile(k, s, h, 0, 0, d, 0)
        for d in NEAR:
            for h in range(2):
                pass_tile(k, s, h, 0, 0, 0, d)

    def gather_rest(k, s):
        arrived(v[s].at[k, pl.ds(0, 2)], near_r.at[k, s])
        for p in (1, 3):
            for d in NEAR:
                for h in range(2):
                    pass_tile(k, s, h, p, 0, 0, d)
        arrived(v[s].at[k, 0], far_r.at[k, s])
        for d in NEAR:
            for h in range(2):
                pass_tile(k, s, h, 2, 0, 0, d)

    def gathered(k, s):
        arrived(v[s].at[k, pl.ds(0, 12)], rest_r.at[k, s])

    def listed(k, s, b):
        return jnp.concatenate([v[s][k, tiles_ref[b, n]] for n in range(LISTED)], axis=0)

    def grid_first(ext):
        for b in range(BATCH):
            both = jnp.concatenate([listed(0, s, b) for s in range(STREAMS)], axis=1)
            waves = jnp.dot(g[b], both, preferred_element_type=F32)
            density = jnp.sum(waves * waves, axis=1, keepdims=True)
            root = jnp.exp(jnp.log(density * (3.0 / jnp.pi)) * (1.0 / 3.0))
            value = jnp.broadcast_to(ext[:, b : b + 1] - root, (PTS, LANES))
            pot[b] = value
            term = (jnp.concatenate([value] * STREAMS, axis=1) * waves).astype(BF)
            sums = jnp.dot(gt[b], term, preferred_element_type=F32)
            for s in range(STREAMS):
                part = sums[:, s * LANES : (s + 1) * LANES]
                yb[s, pl.ds(b * LISTED, LISTED)] = part.reshape(LISTED, TILE, LANES)

    def grid(k, s):
        for b in range(BATCH):
            waves = jnp.dot(g[b], listed(k, s, b), preferred_element_type=F32)
            term = (pot[b] * waves).astype(BF)
            sums = jnp.dot(gt[b], term, preferred_element_type=F32)
            yb[s, pl.ds(b * LISTED, LISTED)] = sums.reshape(LISTED, TILE, LANES)

    def scatter(k, s):
        built = set()

        def build(dy, dz):
            if (dy, dz) in built:
                return
            built.add((dy, dz))
            u = at(dy, dz)
            sb[s, k, u] = (yb[s, inv[0, u]] + yb[s, inv[1, u]]).astype(BF)

        for q in (*FAR, 0):
            for d in FAR:
                build(q, d)
                build(d, q)
                for h in range(2):
                    start(
                        sb.at[s, k, tile_of(h, d, q), pl.ds(h * HALF, HALF)],
                        r1.at[s, k, q, h, 3 - d],
                        r1_s.at[s],
                        r1_r.at[k, s, q],
                        (tile_of(h, d, 0), col),
                    )
        build(0, 0)

    def kinetic(k):
        def block(n, carry):
            rows = pl.ds(pl.multiple_of(n * 256, 256), 256)
            both = jnp.concatenate([v[s][k].reshape(16 * TILE, LANES) for s in range(STREAMS)], axis=1)
            part = jnp.dot(kin[rows, :], both, preferred_element_type=F32).astype(BF)
            for s in range(STREAMS):
                cb[s, k, pl.ds(2 * n, 2)] = part[:, s * LANES : (s + 1) * LANES].reshape(2, TILE, LANES)
            return carry

        lax.fori_loop(0, 4, block, 0)
        other = x * 2 + 1 - core
        for s in range(STREAMS):
            for dx in FAR:
                there = lax.rem(x + dx, 4)
                for e in range(2):
                    start(
                        cb.at[s, k, there * 2 + e],
                        cr.at[s, k, (3 - dx) * 2 + core],
                        c_s.at[s],
                        c_r.at[k, s],
                        (row, there * 2 + e),
                    )
            start(cb.at[s, k, other], cr.at[s, k, 6], c_s.at[s], c_r.at[k, s], (row, other))

    def pass_on(k, s):
        kept = []
        for q in (*FAR, 0):
            arrived(r1.at[s, k, q], r1_r.at[k, s, q])
            for h in range(2):
                own = sb.at[s, k, tile_of(h, 0, q), pl.ds(h * HALF, HALF)]
                total = own[...].astype(F32)
                for n in range(3):
                    total = total + r1[s, k, q, h, n].astype(F32)
                if q == 0:
                    kept.append(total)
                    continue
                own[...] = total.astype(BF)
                start(own, r2.at[s, k, h, 3 - q], r2_s.at[s], r2_r.at[k, s], (tile_of(h, 0, q), col))
        return jnp.concatenate(kept, axis=0)

    def collect(k, s, kept):
        arrived(cr.at[s, k], c_r.at[k, s])
        total = kept + cb[s, k, col].astype(F32)
        for n in range(7):
            total = total + cr[s, k, n].astype(F32)
        arrived(r2.at[s, k], r2_r.at[k, s])
        total = total + sum(
            jnp.concatenate([r2[s, k, h, n].astype(F32) for h in range(2)], axis=0) for n in range(3)
        )
        applied = total / spread - (center / spread) * v[s][k, row].astype(F32)
        if k == 0:
            v[s][1, row] = applied.astype(BF)
            return
        result = 2.0 * applied - v[s][k - 1, row].astype(F32)
        if k == 1:
            v[s][2, row] = result.astype(BF)
        else:
            out_ref[:, pl.ds(s * LANES, LANES)] = result

    kept = {}

    def step(name, k, s):
        with jax.named_scope(f"{name}{k}{s}"):
            if name == "own":
                gather_own(k, s)
            elif name == "rest":
                gather_rest(k, s)
            elif name == "wait":
                gathered(k, s)
            elif name == "grid":
                grid(k, s)
                scatter(k, s)
            elif name == "scat":
                scatter(k, s)
            elif name == "kin":
                kinetic(k)
            elif name == "pass":
                kept[k, s] = pass_on(k, s)
            elif name == "coll":
                collect(k, s, kept[k, s])

    step("own", 0, 0)
    step("own", 0, 1)
    with jax.named_scope("prep"):
        load_g.wait()
        for b in range(BATCH):
            gt[b] = g[b].T
        ext = ext_ref[...]
        ext = jnp.concatenate([ext, ext], axis=0).T
    step("rest", 0, 0)
    step("rest", 0, 1)
    step("wait", 0, 0)
    step("wait", 0, 1)
    with jax.named_scope("first"):
        grid_first(ext)
    for k in range(3):
        if k == 0:
            step("scat", 0, 0)
            step("scat", 0, 1)
            load_k.wait()
        else:
            step("rest", k, 0)
            step("rest", k, 1)
            step("wait", k, 0)
            step("grid", k, 0)
            step("wait", k, 1)
            step("grid", k, 1)
        step("kin", k, 0)
        step("pass", k, 0)
        step("pass", k, 1)
        step("coll", k, 0)
        if k < 2:
            step("own", k + 1, 0)
        step("coll", k, 1)
        if k < 2:
            step("own", k + 1, 1)

    for s in range(STREAMS):
        sent(v[s].at[:, pl.ds(0, 15)], ag_s.at[s])
        sent(r1.at[s], r1_s.at[s])
        sent(r2.at[s], r2_s.at[s])
        sent(cr.at[s], c_s.at[s])


def body(grid_values, external, tiles, kinetic, orbitals):
    any_spec = pl.BlockSpec(memory_space=pl.ANY)
    dma = pltpu.SemaphoreType.DMA
    return pl.pallas_call(
        kernel,
        out_shape=jax.ShapeDtypeStruct((TILE, STREAMS * LANES), F32),
        in_specs=[
            pl.BlockSpec(memory_space=pltpu.SMEM),
            pl.BlockSpec(memory_space=pltpu.VMEM),
            any_spec,
            any_spec,
            any_spec,
        ],
        out_specs=pl.BlockSpec(memory_space=pltpu.VMEM),
        scratch_shapes=[
            pltpu.VMEM(kinetic.shape, BF),
            pltpu.VMEM((BATCH, PTS, LIST), BF),
            pltpu.VMEM((BATCH, LIST, PTS), BF),
            pltpu.VMEM((3, 16, TILE, LANES), BF),
            pltpu.VMEM((3, 16, TILE, LANES), BF),
            pltpu.VMEM((STREAMS, 3, 16, TILE, LANES), BF),
            pltpu.VMEM((STREAMS, 3, 4, 2, 3, HALF, LANES), BF),
            pltpu.VMEM((STREAMS, 3, 2, 3, HALF, LANES), BF),
            pltpu.VMEM((STREAMS, 3, 8, TILE, LANES), BF),
            pltpu.VMEM((STREAMS, 3, 7, TILE, LANES), BF),
            pltpu.VMEM((BATCH, PTS, LANES), F32),
            pltpu.VMEM((STREAMS, SLOTS + 1, TILE, LANES), F32),
            pltpu.SMEM((2, 16), jnp.int32),
            dma((2 + STREAMS,)),
            dma((3, STREAMS)),
            dma((3, STREAMS)),
            dma((3, STREAMS)),
            dma((3, STREAMS, 4)),
            dma((3, STREAMS)),
            dma((3, STREAMS)),
            dma((STREAMS,)),
            dma((STREAMS,)),
            dma((STREAMS,)),
            dma((STREAMS,)),
        ],
        compiler_params=pltpu.CompilerParams(
            collective_id=0, has_side_effects=True, vmem_limit_bytes=60 * 1024 * 1024
        ),
    )(tiles, external, grid_values, kinetic, orbitals)


def solution(mesh):
    return jax.shard_map(
        body,
        mesh=mesh,
        in_specs=(
            P(("row", "col"), None, None),
            P(("row", "col"), None),
            P(("row", "col"), None),
            P("row", "col"),
            P(("row", "col"), None),
        ),
        out_specs=P(("row", "col"), None),
        check_vma=False,
    )
```

```python
import jax
import jax.numpy as jnp
from jax import lax
from jax.experimental import pallas as pl
from jax.experimental.pallas import tpu as pltpu
from jax.sharding import PartitionSpec as P

MESH = pl.DeviceIdType.MESH
TILE = 128
STREAMS = 2
LANES = 128
LISTED = 3
BATCH = 4
PTS = 256
LIST = 384
SLOTS = BATCH * LISTED
HALF = TILE // 2
FAR = (2, 1, 3)
NEAR = (1, 3, 2)
BF = jnp.bfloat16
F32 = jnp.float32
center = 1.0
spread = 2.5


def kernel(
    tiles_hbm, ext_hbm, g_hbm, k_hbm, orb_hbm, out_ref,
    kin, g, gt, v_one, v_two, sb, r1, r2, cb, cr, pot, yb, ext_ref, tiles_ref, inv,
    load_sem, near_r, far_r, rest_r, r1_r, r2_r, c_r, ag_s, r1_s, r2_s, c_s,
):
    v = (v_one, v_two)
    row, col = lax.axis_index("row"), lax.axis_index("col")
    y, z = row // 4, row % 4
    x, core = col // 2, col % 2

    def at(dy, dz):
        return lax.rem(y + dy, 4) * 4 + lax.rem(z + dz, 4)

    def tile_of(h, p, q):
        return at(q, p) if h == 0 else at(p, q)

    def start(src, dst, send, recv, target):
        pltpu.make_async_remote_copy(
            src_ref=src, dst_ref=dst, send_sem=send, recv_sem=recv, device_id=target, device_id_type=MESH
        ).start()

    def arrived(ref, recv):
        pltpu.make_async_remote_copy(
            src_ref=ref, dst_ref=ref, send_sem=recv, recv_sem=recv, device_id=(row, col), device_id_type=MESH
        ).wait_recv()

    def sent(ref, send):
        pltpu.make_async_remote_copy(
            src_ref=ref, dst_ref=ref, send_sem=send, recv_sem=send, device_id=(row, col), device_id_type=MESH
        ).wait_send()

    barrier = pltpu.get_barrier_semaphore()
    peers = [(at(0, d), col) for d in NEAR] + [(at(d, 0), col) for d in NEAR]
    peers += [(row, lax.rem(col + d, 8)) for d in range(1, 8)]
    for peer in peers:
        pl.semaphore_signal(barrier, inc=1, device_id=peer, device_id_type=MESH)

    load_k = pltpu.make_async_copy(k_hbm, kin, load_sem.at[0])
    load_g = pltpu.make_async_copy(g_hbm, g, load_sem.at[1])
    load_v = [
        pltpu.make_async_copy(orb_hbm.at[:, pl.ds(s * LANES, LANES)], v[s].at[0, row], load_sem.at[2 + s])
        for s in range(STREAMS)
    ]
    load_ext = pltpu.make_async_copy(ext_hbm, ext_ref, load_sem.at[2 + STREAMS])
    for load in load_v:
        load.start()
    load_ext.start()
    load_tiles = pltpu.make_async_copy(tiles_hbm, tiles_ref, load_sem.at[3 + STREAMS])
    load_tiles.start()
    load_g.start()
    load_k.start()

    def invert(u, carry):
        first, second = jnp.int32(SLOTS), jnp.int32(SLOTS)
        for n in range(SLOTS):
            hit = tiles_ref[n // LISTED, n % LISTED] == u
            second = jnp.where(hit & (first < SLOTS), n, second)
            first = jnp.where(hit & (first == SLOTS), n, first)
        inv[0, u] = first
        inv[1, u] = second
        return carry

    load_tiles.wait()
    lax.fori_loop(0, 16, invert, 0)
    for s in range(STREAMS):
        yb[s, SLOTS] = jnp.zeros((TILE, LANES), F32)
    pl.semaphore_wait(barrier, len(peers))
    for load in load_v:
        load.wait()

    def pass_tile(k, s, h, p, q, dp, dq):
        part = v[s].at[k, tile_of(h, p, q), pl.ds(h * HALF, HALF)]
        if dq:
            recv = rest_r.at[k, s]
        else:
            recv = far_r.at[k, s] if dp == 2 else near_r.at[k, s]
        start(part, part, ag_s.at[s], recv, (tile_of(h, dp, dq), col))

    def gather_own(k, s):
        for d in FAR:
            for h in range(2):
                pass_tile(k, s, h, 0, 0, d, 0)
        for d in FAR:
            for h in range(2):
                pass_tile(k, s, h, 0, 0, 0, d)

    def gather_rest(k, s):
        arrived(v[s].at[k, pl.ds(0, 2)], near_r.at[k, s])
        for p in (1, 3):
            for d in FAR:
                for h in range(2):
                    pass_tile(k, s, h, p, 0, 0, d)
        arrived(v[s].at[k, 0], far_r.at[k, s])
        for d in FAR:
            for h in range(2):
                pass_tile(k, s, h, 2, 0, 0, d)

    def gathered(k, s):
        arrived(v[s].at[k, pl.ds(0, 12)], rest_r.at[k, s])

    def listed(k, s, b):
        return jnp.concatenate([v[s][k, tiles_ref[b, n]] for n in range(LISTED)], axis=0)

    def grid_first(ext):
        terms = []
        waves = [
            jnp.dot(
                g[b],
                jnp.concatenate([listed(0, s, b) for s in range(STREAMS)], axis=1),
                preferred_element_type=F32,
            )
            for b in range(BATCH)
        ]
        for b in range(BATCH):
            density = jnp.sum(waves[b] * waves[b], axis=1, keepdims=True)
            root = jnp.exp(jnp.log(density * (3.0 / jnp.pi)) * (1.0 / 3.0))
            value = jnp.broadcast_to(ext[:, b : b + 1] - root, (PTS, LANES))
            pot[b] = value
            terms.append((jnp.concatenate([value] * STREAMS, axis=1) * waves[b]).astype(BF))
        for b in range(BATCH):
            sums = jnp.dot(gt[b], terms[b], preferred_element_type=F32)
            for s in range(STREAMS):
                part = sums[:, s * LANES : (s + 1) * LANES]
                yb[s, pl.ds(b * LISTED, LISTED)] = part.reshape(LISTED, TILE, LANES)

    def grid(k, s):
        waves = [jnp.dot(g[b], listed(k, s, b), preferred_element_type=F32) for b in range(BATCH)]
        terms = [(pot[b] * waves[b]).astype(BF) for b in range(BATCH)]
        for b in range(BATCH):
            sums = jnp.dot(gt[b], terms[b], preferred_element_type=F32)
            yb[s, pl.ds(b * LISTED, LISTED)] = sums.reshape(LISTED, TILE, LANES)

    def scatter(k, s):
        built = set()

        def build(dy, dz):
            if (dy, dz) in built:
                return
            built.add((dy, dz))
            u = at(dy, dz)
            sb[s, k, u] = (yb[s, inv[0, u]] + yb[s, inv[1, u]]).astype(BF)

        for q in (*FAR, 0):
            for d in FAR:
                build(q, d)
                build(d, q)
                for h in range(2):
                    start(
                        sb.at[s, k, tile_of(h, d, q), pl.ds(h * HALF, HALF)],
                        r1.at[s, k, q, h, 3 - d],
                        r1_s.at[s],
                        r1_r.at[k, s, q],
                        (tile_of(h, d, 0), col),
                    )
        build(0, 0)

    def send_parts(k, s):
        for dx in FAR:
            there = lax.rem(x + dx, 4)
            for e in range(2):
                start(
                    cb.at[s, k, there * 2 + e],
                    cr.at[s, k, (3 - dx) * 2 + core],
                    c_s.at[s],
                    c_r.at[k, s],
                    (row, there * 2 + e),
                )
        other = x * 2 + 1 - core
        start(cb.at[s, k, other], cr.at[s, k, 6], c_s.at[s], c_r.at[k, s], (row, other))

    def kinetic(k, streams):
        def block(n, carry):
            rows = pl.ds(pl.multiple_of(n * 256, 256), 256)
            right = jnp.concatenate([v[s][k].reshape(16 * TILE, LANES) for s in streams], axis=1)
            part = jnp.dot(kin[rows, :], right, preferred_element_type=F32).astype(BF)
            for i, s in enumerate(streams):
                cb[s, k, pl.ds(2 * n, 2)] = part[:, i * LANES : (i + 1) * LANES].reshape(2, TILE, LANES)
            return carry

        lax.fori_loop(0, 4, block, 0)
        for s in streams:
            send_parts(k, s)

    def pass_on(k, s):
        kept = []
        for q in (*FAR, 0):
            arrived(r1.at[s, k, q], r1_r.at[k, s, q])
            for h in range(2):
                own = sb.at[s, k, tile_of(h, 0, q), pl.ds(h * HALF, HALF)]
                total = own[...].astype(F32)
                for n in range(3):
                    total = total + r1[s, k, q, h, n].astype(F32)
                if q == 0:
                    kept.append(total)
                    continue
                own[...] = total.astype(BF)
                start(own, r2.at[s, k, h, 3 - q], r2_s.at[s], r2_r.at[k, s], (tile_of(h, 0, q), col))
        return jnp.concatenate(kept, axis=0)

    def collect(k, s, kept):
        arrived(cr.at[s, k], c_r.at[k, s])
        total = kept + cb[s, k, col].astype(F32)
        for n in range(7):
            total = total + cr[s, k, n].astype(F32)
        arrived(r2.at[s, k], r2_r.at[k, s])
        total = total + sum(
            jnp.concatenate([r2[s, k, h, n].astype(F32) for h in range(2)], axis=0) for n in range(3)
        )
        applied = total / spread - (center / spread) * v[s][k, row].astype(F32)
        if k == 0:
            v[s][1, row] = applied.astype(BF)
            return
        result = 2.0 * applied - v[s][k - 1, row].astype(F32)
        if k == 1:
            v[s][2, row] = result.astype(BF)
        else:
            out_ref[:, pl.ds(s * LANES, LANES)] = result

    kept = {}

    def step(name, k, s):
        with jax.named_scope(f"{name}{k}{s}"):
            if name == "own":
                gather_own(k, s)
            elif name == "rest":
                gather_rest(k, s)
            elif name == "wait":
                gathered(k, s)
            elif name == "grid":
                grid(k, s)
                scatter(k, s)
            elif name == "scat":
                scatter(k, s)
            elif name == "kin":
                kinetic(k, (0, 1) if k == 0 else (s,))
            elif name == "pass":
                kept[k, s] = pass_on(k, s)
            elif name == "coll":
                collect(k, s, kept[k, s])

    step("own", 0, 0)
    step("own", 0, 1)
    with jax.named_scope("prep"):
        load_g.wait()
        for b in range(BATCH):
            gt[b] = g[b].T
        load_ext.wait()
        ext = ext_ref[...]
        ext = jnp.concatenate([ext, ext], axis=0).T
    step("rest", 0, 0)
    step("rest", 0, 1)
    step("wait", 0, 0)
    step("wait", 0, 1)
    with jax.named_scope("first"):
        grid_first(ext)
    for k in range(3):
        if k == 0:
            step("scat", 0, 0)
            step("scat", 0, 1)
            load_k.wait()
            step("kin", 0, 0)
        else:
            step("rest", k, 0)
            step("rest", k, 1)
            step("wait", k, 0)
            step("grid", k, 0)
            step("kin", k, 0)
            step("wait", k, 1)
            step("grid", k, 1)
            step("kin", k, 1)
        step("pass", k, 0)
        step("pass", k, 1)
        step("coll", k, 0)
        if k < 2:
            step("own", k + 1, 0)
        step("coll", k, 1)
        if k < 2:
            step("own", k + 1, 1)

    for s in range(STREAMS):
        sent(v[s].at[:, pl.ds(0, 15)], ag_s.at[s])
        sent(r1.at[s], r1_s.at[s])
        sent(r2.at[s], r2_s.at[s])
        sent(cr.at[s], c_s.at[s])


def body(grid_values, external, tiles, kinetic, orbitals):
    any_spec = pl.BlockSpec(memory_space=pl.ANY)
    dma = pltpu.SemaphoreType.DMA
    return pl.pallas_call(
        kernel,
        out_shape=jax.ShapeDtypeStruct((TILE, STREAMS * LANES), F32),
        in_specs=[
            any_spec,
            any_spec,
            any_spec,
            any_spec,
            any_spec,
        ],
        out_specs=pl.BlockSpec(memory_space=pltpu.VMEM),
        scratch_shapes=[
            pltpu.VMEM(kinetic.shape, BF),
            pltpu.VMEM((BATCH, PTS, LIST), BF),
            pltpu.VMEM((BATCH, LIST, PTS), BF),
            pltpu.VMEM((3, 16, TILE, LANES), BF),
            pltpu.VMEM((3, 16, TILE, LANES), BF),
            pltpu.VMEM((STREAMS, 3, 16, TILE, LANES), BF),
            pltpu.VMEM((STREAMS, 3, 4, 2, 3, HALF, LANES), BF),
            pltpu.VMEM((STREAMS, 3, 2, 3, HALF, LANES), BF),
            pltpu.VMEM((STREAMS, 3, 8, TILE, LANES), BF),
            pltpu.VMEM((STREAMS, 3, 7, TILE, LANES), BF),
            pltpu.VMEM((BATCH, PTS, LANES), F32),
            pltpu.VMEM((STREAMS, SLOTS + 1, TILE, LANES), F32),
            pltpu.VMEM((BATCH, PTS), F32),
            pltpu.SMEM((BATCH, LISTED), jnp.int32),
            pltpu.SMEM((2, 16), jnp.int32),
            dma((4 + STREAMS,)),
            dma((3, STREAMS)),
            dma((3, STREAMS)),
            dma((3, STREAMS)),
            dma((3, STREAMS, 4)),
            dma((3, STREAMS)),
            dma((3, STREAMS)),
            dma((STREAMS,)),
            dma((STREAMS,)),
            dma((STREAMS,)),
            dma((STREAMS,)),
        ],
        compiler_params=pltpu.CompilerParams(
            collective_id=0, has_side_effects=True, vmem_limit_bytes=60 * 1024 * 1024
        ),
    )(tiles, external, grid_values, kinetic, orbitals)


def solution(mesh):
    return jax.shard_map(
        body,
        mesh=mesh,
        in_specs=(
            P(("row", "col"), None, None),
            P(("row", "col"), None),
            P(("row", "col"), None),
            P("row", "col"),
            P(("row", "col"), None),
        ),
        out_specs=P(("row", "col"), None),
        check_vma=False,
    )
```

```python
import jax
import jax.numpy as jnp
from jax import lax
from jax.experimental import pallas as pl
from jax.experimental.pallas import tpu as pltpu
from jax.sharding import PartitionSpec as P

MESH = pl.DeviceIdType.MESH
TILE = 128
STREAMS = 2
LANES = 128
LISTED = 3
BATCH = 4
PTS = 256
LIST = 384
SLOTS = BATCH * LISTED
HALF = TILE // 2
FAR = (2, 1, 3)
NEAR = (1, 3, 2)
BF = jnp.bfloat16
F32 = jnp.float32
center = 1.0
spread = 2.5


def kernel(
    tiles_hbm, ext_hbm, g_hbm, k_hbm, orb_hbm, out_ref, prev_ref,
    kin, g, gt, v_one, v_two, sb, r1, r2, cb, cr, pot, yb, ext_ref, tiles_ref, inv,
    load_sem, near_r, far_r, rest_r, r1_r, r2_r, c_r, ag_s, r1_s, r2_s, c_s,
):
    v = (v_one, v_two)
    row, col = lax.axis_index("row"), lax.axis_index("col")
    y, z = row // 4, row % 4
    x, core = col // 2, col % 2

    def at(dy, dz):
        return lax.rem(y + dy, 4) * 4 + lax.rem(z + dz, 4)

    def tile_of(h, p, q):
        return at(q, p) if h == 0 else at(p, q)

    def start(src, dst, send, recv, target):
        pltpu.make_async_remote_copy(
            src_ref=src, dst_ref=dst, send_sem=send, recv_sem=recv, device_id=target, device_id_type=MESH
        ).start()

    def arrived(ref, recv):
        pltpu.make_async_remote_copy(
            src_ref=ref, dst_ref=ref, send_sem=recv, recv_sem=recv, device_id=(row, col), device_id_type=MESH
        ).wait_recv()

    def sent(ref, send):
        pltpu.make_async_remote_copy(
            src_ref=ref, dst_ref=ref, send_sem=send, recv_sem=send, device_id=(row, col), device_id_type=MESH
        ).wait_send()

    barrier = pltpu.get_barrier_semaphore()
    peers = [(at(0, d), col) for d in NEAR] + [(at(d, 0), col) for d in NEAR]
    peers += [(row, lax.rem(col + d, 8)) for d in range(1, 8)]
    for peer in peers:
        pl.semaphore_signal(barrier, inc=1, device_id=peer, device_id_type=MESH)

    load_k = pltpu.make_async_copy(k_hbm, kin, load_sem.at[0])
    load_g = pltpu.make_async_copy(g_hbm, g, load_sem.at[1])
    load_v = [
        pltpu.make_async_copy(orb_hbm.at[:, pl.ds(s * LANES, LANES)], v[s].at[0, row], load_sem.at[2 + s])
        for s in range(STREAMS)
    ]
    load_ext = pltpu.make_async_copy(ext_hbm, ext_ref, load_sem.at[2 + STREAMS])
    for load in load_v:
        load.start()
    load_ext.start()
    load_tiles = pltpu.make_async_copy(tiles_hbm, tiles_ref, load_sem.at[3 + STREAMS])
    load_tiles.start()
    load_g.start()
    load_k.start()

    def invert(u, carry):
        first, second = jnp.int32(SLOTS), jnp.int32(SLOTS)
        for n in range(SLOTS):
            hit = tiles_ref[n // LISTED, n % LISTED] == u
            second = jnp.where(hit & (first < SLOTS), n, second)
            first = jnp.where(hit & (first == SLOTS), n, first)
        inv[0, u] = first
        inv[1, u] = second
        return carry

    load_tiles.wait()
    lax.fori_loop(0, 16, invert, 0)
    for s in range(STREAMS):
        yb[s, SLOTS] = jnp.zeros((TILE, LANES), F32)
    pl.semaphore_wait(barrier, len(peers))
    for load in load_v:
        load.wait()

    def pass_tile(k, s, h, p, q, dp, dq):
        part = v[s].at[k, tile_of(h, p, q), pl.ds(h * HALF, HALF)]
        if dq:
            recv = rest_r.at[k, s]
        else:
            recv = far_r.at[k, s] if dp == 2 else near_r.at[k, s]
        start(part, part, ag_s.at[s], recv, (tile_of(h, dp, dq), col))

    def gather_own(k, s):
        for d in FAR:
            for h in range(2):
                pass_tile(k, s, h, 0, 0, d, 0)
        for d in FAR:
            for h in range(2):
                pass_tile(k, s, h, 0, 0, 0, d)

    def gather_rest(k, s):
        arrived(v[s].at[k, pl.ds(0, 2)], near_r.at[k, s])
        for p in (1, 3):
            for d in FAR:
                for h in range(2):
                    pass_tile(k, s, h, p, 0, 0, d)
        arrived(v[s].at[k, 0], far_r.at[k, s])
        for d in FAR:
            for h in range(2):
                pass_tile(k, s, h, 2, 0, 0, d)

    def gathered(k, s):
        arrived(v[s].at[k, pl.ds(0, 12)], rest_r.at[k, s])

    def listed(k, s, b):
        return jnp.concatenate([v[s][k, tiles_ref[b, n]] for n in range(LISTED)], axis=0)

    def grid_first(ext):
        terms = []
        waves = [
            jnp.dot(
                g[b],
                jnp.concatenate([listed(0, s, b) for s in range(STREAMS)], axis=1),
                preferred_element_type=F32,
            )
            for b in range(BATCH)
        ]
        for b in range(BATCH):
            density = jnp.sum(waves[b] * waves[b], axis=1, keepdims=True)
            root = jnp.exp(jnp.log(density * (3.0 / jnp.pi)) * (1.0 / 3.0))
            value = jnp.broadcast_to(ext[:, b : b + 1] - root, (PTS, LANES))
            pot[b] = value
            terms.append((jnp.concatenate([value] * STREAMS, axis=1) * waves[b]).astype(BF))
        for b in range(BATCH):
            sums = jnp.dot(gt[b], terms[b], preferred_element_type=F32)
            for s in range(STREAMS):
                part = sums[:, s * LANES : (s + 1) * LANES]
                yb[s, pl.ds(b * LISTED, LISTED)] = part.reshape(LISTED, TILE, LANES)

    def grid(k, s):
        waves = [jnp.dot(g[b], listed(k, s, b), preferred_element_type=F32) for b in range(BATCH)]
        terms = [(pot[b] * waves[b]).astype(BF) for b in range(BATCH)]
        for b in range(BATCH):
            sums = jnp.dot(gt[b], terms[b], preferred_element_type=F32)
            yb[s, pl.ds(b * LISTED, LISTED)] = sums.reshape(LISTED, TILE, LANES)

    def scatter(k, s):
        built = set()

        def build(dy, dz):
            if (dy, dz) in built:
                return
            built.add((dy, dz))
            u = at(dy, dz)
            sb[s, k, u] = (yb[s, inv[0, u]] + yb[s, inv[1, u]]).astype(BF)

        for q in (*FAR, 0):
            for d in FAR:
                build(q, d)
                build(d, q)
                for h in range(2):
                    start(
                        sb.at[s, k, tile_of(h, d, q), pl.ds(h * HALF, HALF)],
                        r1.at[s, k, q, h, 3 - d],
                        r1_s.at[s],
                        r1_r.at[k, s, q],
                        (tile_of(h, d, 0), col),
                    )
        build(0, 0)

    def send_parts(k, s):
        for dx in FAR:
            there = lax.rem(x + dx, 4)
            for e in range(2):
                start(
                    cb.at[s, k, there * 2 + e],
                    cr.at[s, k, (3 - dx) * 2 + core],
                    c_s.at[s],
                    c_r.at[k, s],
                    (row, there * 2 + e),
                )
        other = x * 2 + 1 - core
        start(cb.at[s, k, other], cr.at[s, k, 6], c_s.at[s], c_r.at[k, s], (row, other))

    def kinetic(k, streams):
        def block(n, carry):
            rows = pl.ds(pl.multiple_of(n * 512, 512), 512)
            right = jnp.concatenate([v[s][k].reshape(16 * TILE, LANES) for s in streams], axis=1)
            part = jnp.dot(kin[rows, :], right, preferred_element_type=F32).astype(BF)
            for i, s in enumerate(streams):
                cb[s, k, pl.ds(4 * n, 4)] = part[:, i * LANES : (i + 1) * LANES].reshape(4, TILE, LANES)
            return carry

        lax.fori_loop(0, 2, block, 0)
        for s in streams:
            send_parts(k, s)

    def pass_on(k, s):
        kept = []
        for q in (*FAR, 0):
            arrived(r1.at[s, k, q], r1_r.at[k, s, q])
            for h in range(2):
                own = sb.at[s, k, tile_of(h, 0, q), pl.ds(h * HALF, HALF)]
                total = own[...].astype(F32)
                for n in range(3):
                    total = total + r1[s, k, q, h, n].astype(F32)
                if q == 0:
                    kept.append(total)
                    continue
                own[...] = total.astype(BF)
                start(own, r2.at[s, k, h, 3 - q], r2_s.at[s], r2_r.at[k, s], (tile_of(h, 0, q), col))
        return jnp.concatenate(kept, axis=0)

    def collect(k, s, kept):
        arrived(cr.at[s, k], c_r.at[k, s])
        total = kept + cb[s, k, col].astype(F32)
        for n in range(7):
            total = total + cr[s, k, n].astype(F32)
        arrived(r2.at[s, k], r2_r.at[k, s])
        total = total + sum(
            jnp.concatenate([r2[s, k, h, n].astype(F32) for h in range(2)], axis=0) for n in range(3)
        )
        applied = total / spread - (center / spread) * v[s][k, row].astype(F32)
        if k == 0:
            v[s][1, row] = applied.astype(BF)
            return
        if k == 1:
            v[s][2, row] = (2.0 * applied - v[s][0, row].astype(F32)).astype(BF)
        else:
            out_ref[:, pl.ds(s * LANES, LANES)] = 2.0 * applied
            prev_ref[:, pl.ds(s * LANES, LANES)] = v[s][1, row]

    kept = {}

    def step(name, k, s):
        with jax.named_scope(f"{name}{k}{s}"):
            if name == "own":
                gather_own(k, s)
            elif name == "rest":
                gather_rest(k, s)
            elif name == "wait":
                gathered(k, s)
            elif name == "grid":
                grid(k, s)
                scatter(k, s)
            elif name == "scat":
                scatter(k, s)
            elif name == "kin":
                kinetic(k, (0, 1) if k == 0 else (s,))
            elif name == "pass":
                kept[k, s] = pass_on(k, s)
            elif name == "coll":
                collect(k, s, kept[k, s])

    step("own", 0, 0)
    step("own", 0, 1)
    with jax.named_scope("prep"):
        load_g.wait()
        for b in range(BATCH):
            gt[b] = g[b].T
        load_ext.wait()
        ext = ext_ref[...]
        ext = jnp.concatenate([ext, ext], axis=0).T
    step("rest", 0, 0)
    step("rest", 0, 1)
    step("wait", 0, 0)
    step("wait", 0, 1)
    with jax.named_scope("first"):
        grid_first(ext)
    for k in range(3):
        if k == 0:
            step("scat", 0, 0)
            step("scat", 0, 1)
            load_k.wait()
            step("kin", 0, 0)
        else:
            step("rest", k, 0)
            step("rest", k, 1)
            step("wait", k, 0)
            step("grid", k, 0)
            step("kin", k, 0)
            step("wait", k, 1)
            step("grid", k, 1)
            step("kin", k, 1)
        step("pass", k, 0)
        step("pass", k, 1)
        step("coll", k, 0)
        if k < 2:
            step("own", k + 1, 0)
        step("coll", k, 1)
        if k < 2:
            step("own", k + 1, 1)

    for s in range(STREAMS):
        sent(v[s].at[:, pl.ds(0, 15)], ag_s.at[s])
        sent(r1.at[s], r1_s.at[s])
        sent(r2.at[s], r2_s.at[s])
        sent(cr.at[s], c_s.at[s])


def body(grid_values, external, tiles, kinetic, orbitals):
    any_spec = pl.BlockSpec(memory_space=pl.ANY)
    dma = pltpu.SemaphoreType.DMA
    doubled, before = pl.pallas_call(
        kernel,
        out_shape=[
            jax.ShapeDtypeStruct((TILE, STREAMS * LANES), F32),
            jax.ShapeDtypeStruct((TILE, STREAMS * LANES), BF),
        ],
        in_specs=[
            any_spec,
            any_spec,
            any_spec,
            any_spec,
            any_spec,
        ],
        out_specs=[pl.BlockSpec(memory_space=pltpu.VMEM)] * 2,
        scratch_shapes=[
            pltpu.VMEM(kinetic.shape, BF),
            pltpu.VMEM((BATCH, PTS, LIST), BF),
            pltpu.VMEM((BATCH, LIST, PTS), BF),
            pltpu.VMEM((3, 16, TILE, LANES), BF),
            pltpu.VMEM((3, 16, TILE, LANES), BF),
            pltpu.VMEM((STREAMS, 3, 16, TILE, LANES), BF),
            pltpu.VMEM((STREAMS, 3, 4, 2, 3, HALF, LANES), BF),
            pltpu.VMEM((STREAMS, 3, 2, 3, HALF, LANES), BF),
            pltpu.VMEM((STREAMS, 3, 8, TILE, LANES), BF),
            pltpu.VMEM((STREAMS, 3, 7, TILE, LANES), BF),
            pltpu.VMEM((BATCH, PTS, LANES), F32),
            pltpu.VMEM((STREAMS, SLOTS + 1, TILE, LANES), F32),
            pltpu.VMEM((BATCH, PTS), F32),
            pltpu.SMEM((BATCH, LISTED), jnp.int32),
            pltpu.SMEM((2, 16), jnp.int32),
            dma((4 + STREAMS,)),
            dma((3, STREAMS)),
            dma((3, STREAMS)),
            dma((3, STREAMS)),
            dma((3, STREAMS, 4)),
            dma((3, STREAMS)),
            dma((3, STREAMS)),
            dma((STREAMS,)),
            dma((STREAMS,)),
            dma((STREAMS,)),
            dma((STREAMS,)),
        ],
        compiler_params=pltpu.CompilerParams(
            collective_id=0, has_side_effects=True, vmem_limit_bytes=62914560
        ),
    )(tiles, external, grid_values, kinetic, orbitals)
    return doubled - before.astype(F32)


def solution(mesh):
    return jax.shard_map(
        body,
        mesh=mesh,
        in_specs=(
            P(("row", "col"), None, None),
            P(("row", "col"), None),
            P(("row", "col"), None),
            P("row", "col"),
            P(("row", "col"), None),
        ),
        out_specs=P(("row", "col"), None),
        check_vma=False,
    )
```

```python
import jax
import jax.numpy as jnp
from jax import lax
from jax.experimental import pallas as pl
from jax.experimental.pallas import tpu as pltpu
from jax.sharding import PartitionSpec as P

MESH = pl.DeviceIdType.MESH
TILE = 128
STREAMS = 2
LANES = 128
LISTED = 3
BATCH = 4
PTS = 256
LIST = 384
SLOTS = BATCH * LISTED
HALF = TILE // 2
FAR = (2, 1, 3)
NEAR = (1, 3, 2)
BF = jnp.bfloat16
F32 = jnp.float32
center = 1.0
spread = 2.5


def kernel(
    tiles_hbm, ext_hbm, g_hbm, k_hbm, orb_hbm, out_ref,
    kin, g, gt, v_one, v_two, sb, r1, r2, cb, cr, pot, yb, ext_ref, tiles_ref, inv,
    load_sem, near_r, far_r, rest_r, r1_r, r2_r, c_r, ag_s, r1_s, r2_s, c_s,
):
    v = (v_one, v_two)
    row, col = lax.axis_index("row"), lax.axis_index("col")
    y, z = row // 4, row % 4
    x, core = col // 2, col % 2

    def at(dy, dz):
        return lax.rem(y + dy, 4) * 4 + lax.rem(z + dz, 4)

    def tile_of(h, p, q):
        return at(q, p) if h == 0 else at(p, q)

    def start(src, dst, send, recv, target):
        pltpu.make_async_remote_copy(
            src_ref=src, dst_ref=dst, send_sem=send, recv_sem=recv, device_id=target, device_id_type=MESH
        ).start()

    def arrived(ref, recv):
        pltpu.make_async_remote_copy(
            src_ref=ref, dst_ref=ref, send_sem=recv, recv_sem=recv, device_id=(row, col), device_id_type=MESH
        ).wait_recv()

    def sent(ref, send):
        pltpu.make_async_remote_copy(
            src_ref=ref, dst_ref=ref, send_sem=send, recv_sem=send, device_id=(row, col), device_id_type=MESH
        ).wait_send()

    barrier = pltpu.get_barrier_semaphore()
    peers = [(at(0, d), col) for d in NEAR] + [(at(d, 0), col) for d in NEAR]
    peers += [(row, lax.rem(col + d, 8)) for d in range(1, 8)]
    for peer in peers:
        pl.semaphore_signal(barrier, inc=1, device_id=peer, device_id_type=MESH)

    load_k = pltpu.make_async_copy(k_hbm, kin, load_sem.at[0])
    load_g = pltpu.make_async_copy(g_hbm, g, load_sem.at[1])
    load_v = [
        pltpu.make_async_copy(orb_hbm.at[:, pl.ds(s * LANES, LANES)], v[s].at[0, row], load_sem.at[2 + s])
        for s in range(STREAMS)
    ]
    load_ext = pltpu.make_async_copy(ext_hbm, ext_ref, load_sem.at[2 + STREAMS])
    for load in load_v:
        load.start()
    load_ext.start()
    load_tiles = pltpu.make_async_copy(tiles_hbm, tiles_ref, load_sem.at[3 + STREAMS])
    load_tiles.start()
    load_g.start()
    load_k.start()

    def invert(u, carry):
        first, second = jnp.int32(SLOTS), jnp.int32(SLOTS)
        for n in range(SLOTS):
            hit = tiles_ref[n // LISTED, n % LISTED] == u
            second = jnp.where(hit & (first < SLOTS), n, second)
            first = jnp.where(hit & (first == SLOTS), n, first)
        inv[0, u] = first
        inv[1, u] = second
        return carry

    load_tiles.wait()
    lax.fori_loop(0, 16, invert, 0)
    for s in range(STREAMS):
        yb[s, SLOTS] = jnp.zeros((TILE, LANES), F32)
    pl.semaphore_wait(barrier, len(peers))
    for load in load_v:
        load.wait()

    def pass_tile(k, s, h, p, q, dp, dq):
        part = v[s].at[k, tile_of(h, p, q), pl.ds(h * HALF, HALF)]
        if dq:
            recv = rest_r.at[k, s]
        else:
            recv = far_r.at[k, s] if dp == 2 else near_r.at[k, s]
        start(part, part, ag_s.at[s], recv, (tile_of(h, dp, dq), col))

    def gather_own(k, s):
        for d in FAR:
            for h in range(2):
                pass_tile(k, s, h, 0, 0, d, 0)
        for d in FAR:
            for h in range(2):
                pass_tile(k, s, h, 0, 0, 0, d)

    def gather_rest(k, s):
        arrived(v[s].at[k, pl.ds(0, 2)], near_r.at[k, s])
        for p in (1, 3):
            for d in FAR:
                for h in range(2):
                    pass_tile(k, s, h, p, 0, 0, d)
        arrived(v[s].at[k, 0], far_r.at[k, s])
        for d in FAR:
            for h in range(2):
                pass_tile(k, s, h, 2, 0, 0, d)

    def gathered(k, s):
        arrived(v[s].at[k, pl.ds(0, 12)], rest_r.at[k, s])

    def listed(k, s, b):
        return jnp.concatenate([v[s][k, tiles_ref[b, n]] for n in range(LISTED)], axis=0)

    def grid_first(ext):
        terms = []
        waves = [
            jnp.dot(
                g[b],
                jnp.concatenate([listed(0, s, b) for s in range(STREAMS)], axis=1),
                preferred_element_type=F32,
            )
            for b in range(BATCH)
        ]
        for b in range(BATCH):
            density = jnp.sum(waves[b] * waves[b], axis=1, keepdims=True)
            root = jnp.exp(jnp.log(density * (3.0 / jnp.pi)) * (1.0 / 3.0))
            value = jnp.broadcast_to(ext[:, b : b + 1] - root, (PTS, LANES))
            pot[b] = value
            terms.append((jnp.concatenate([value] * STREAMS, axis=1) * waves[b]).astype(BF))
        for b in range(BATCH):
            sums = jnp.dot(gt[b], terms[b], preferred_element_type=F32)
            for s in range(STREAMS):
                part = sums[:, s * LANES : (s + 1) * LANES]
                yb[s, pl.ds(b * LISTED, LISTED)] = part.reshape(LISTED, TILE, LANES)

    def grid(k, s):
        waves = [jnp.dot(g[b], listed(k, s, b), preferred_element_type=F32) for b in range(BATCH)]
        terms = [(pot[b] * waves[b]).astype(BF) for b in range(BATCH)]
        for b in range(BATCH):
            sums = jnp.dot(gt[b], terms[b], preferred_element_type=F32)
            yb[s, pl.ds(b * LISTED, LISTED)] = sums.reshape(LISTED, TILE, LANES)

    def scatter(k, s):
        built = set()

        def build(dy, dz):
            if (dy, dz) in built:
                return
            built.add((dy, dz))
            u = at(dy, dz)
            sb[s, k, u] = (yb[s, inv[0, u]] + yb[s, inv[1, u]]).astype(BF)

        for q in (*FAR, 0):
            for d in FAR:
                build(q, d)
                build(d, q)
                for h in range(2):
                    start(
                        sb.at[s, k, tile_of(h, d, q), pl.ds(h * HALF, HALF)],
                        r1.at[s, k, q, h, 3 - d],
                        r1_s.at[s],
                        r1_r.at[k, s, q],
                        (tile_of(h, d, 0), col),
                    )
        build(0, 0)

    def send_parts(k, s):
        for dx in FAR:
            there = lax.rem(x + dx, 4)
            for e in range(2):
                start(
                    cb.at[s, k, there * 2 + e],
                    cr.at[s, k, (3 - dx) * 2 + core],
                    c_s.at[s],
                    c_r.at[k, s],
                    (row, there * 2 + e),
                )
        other = x * 2 + 1 - core
        start(cb.at[s, k, other], cr.at[s, k, 6], c_s.at[s], c_r.at[k, s], (row, other))

    def kinetic(k, streams):
        def block(n, carry):
            rows = pl.ds(pl.multiple_of(n * 256, 256), 256)
            right = jnp.concatenate([v[s][k].reshape(16 * TILE, LANES) for s in streams], axis=1)
            part = jnp.dot(kin[rows, :], right, preferred_element_type=F32).astype(BF)
            for i, s in enumerate(streams):
                cb[s, k, pl.ds(2 * n, 2)] = part[:, i * LANES : (i + 1) * LANES].reshape(2, TILE, LANES)
            return carry

        lax.fori_loop(0, 4, block, 0)
        for s in streams:
            send_parts(k, s)

    def pass_on(k, s):
        for q in FAR:
            arrived(r1.at[s, k, q], r1_r.at[k, s, q])
            for h in range(2):
                own = sb.at[s, k, tile_of(h, 0, q), pl.ds(h * HALF, HALF)]
                total = own[...].astype(F32)
                for n in range(3):
                    total = total + r1[s, k, q, h, n].astype(F32)
                own[...] = total.astype(BF)
                start(own, r2.at[s, k, h, 3 - q], r2_s.at[s], r2_r.at[k, s], (tile_of(h, 0, q), col))

    def keep(k, s):
        arrived(r1.at[s, k, 0], r1_r.at[k, s, 0])
        halves = []
        for h in range(2):
            total = sb[s, k, row, pl.ds(h * HALF, HALF)].astype(F32)
            for n in range(3):
                total = total + r1[s, k, 0, h, n].astype(F32)
            halves.append(total)
        return jnp.concatenate(halves, axis=0)

    def collect(k, s):
        total = keep(k, s)
        arrived(cr.at[s, k], c_r.at[k, s])
        total = total + cb[s, k, col].astype(F32)
        for n in range(7):
            total = total + cr[s, k, n].astype(F32)
        arrived(r2.at[s, k], r2_r.at[k, s])
        total = total + sum(
            jnp.concatenate([r2[s, k, h, n].astype(F32) for h in range(2)], axis=0) for n in range(3)
        )
        applied = total / spread - (center / spread) * v[s][k, row].astype(F32)
        if k == 0:
            v[s][1, row] = applied.astype(BF)
            return
        result = 2.0 * applied - v[s][k - 1, row].astype(F32)
        if k == 1:
            v[s][2, row] = result.astype(BF)
        else:
            out_ref[:, pl.ds(s * LANES, LANES)] = result

    def step(name, k, s):
        with jax.named_scope(f"{name}{k}{s}"):
            if name == "own":
                gather_own(k, s)
            elif name == "rest":
                gather_rest(k, s)
            elif name == "wait":
                gathered(k, s)
            elif name == "grid":
                grid(k, s)
                scatter(k, s)
            elif name == "scat":
                scatter(k, s)
            elif name == "kin":
                kinetic(k, (0, 1) if k == 0 else (s,))
            elif name == "pass":
                pass_on(k, s)
            elif name == "coll":
                collect(k, s)

    step("own", 0, 0)
    step("own", 0, 1)
    with jax.named_scope("prep"):
        load_g.wait()
        for b in range(BATCH):
            gt[b] = g[b].T
        load_ext.wait()
        ext = ext_ref[...]
        ext = jnp.concatenate([ext, ext], axis=0).T
    step("rest", 0, 0)
    step("rest", 0, 1)
    step("wait", 0, 0)
    step("wait", 0, 1)
    with jax.named_scope("first"):
        grid_first(ext)
    for k in range(3):
        if k == 0:
            step("scat", 0, 0)
            step("scat", 0, 1)
            load_k.wait()
            step("kin", 0, 0)
        else:
            step("rest", k, 0)
            step("rest", k, 1)
            step("wait", k, 0)
            step("grid", k, 0)
            step("kin", k, 0)
            step("wait", k, 1)
            step("grid", k, 1)
            step("kin", k, 1)
        step("pass", k, 0)
        step("pass", k, 1)
        step("coll", k, 0)
        if k < 2:
            step("own", k + 1, 0)
        step("coll", k, 1)
        if k < 2:
            step("own", k + 1, 1)

    for s in range(STREAMS):
        sent(v[s].at[:, pl.ds(0, 15)], ag_s.at[s])
        sent(r1.at[s], r1_s.at[s])
        sent(r2.at[s], r2_s.at[s])
        sent(cr.at[s], c_s.at[s])


def body(grid_values, external, tiles, kinetic, orbitals):
    any_spec = pl.BlockSpec(memory_space=pl.ANY)
    dma = pltpu.SemaphoreType.DMA
    return pl.pallas_call(
        kernel,
        out_shape=jax.ShapeDtypeStruct((TILE, STREAMS * LANES), F32),
        in_specs=[
            any_spec,
            any_spec,
            any_spec,
            any_spec,
            any_spec,
        ],
        out_specs=pl.BlockSpec(memory_space=pltpu.VMEM),
        scratch_shapes=[
            pltpu.VMEM(kinetic.shape, BF),
            pltpu.VMEM((BATCH, PTS, LIST), BF),
            pltpu.VMEM((BATCH, LIST, PTS), BF),
            pltpu.VMEM((3, 16, TILE, LANES), BF),
            pltpu.VMEM((3, 16, TILE, LANES), BF),
            pltpu.VMEM((STREAMS, 3, 16, TILE, LANES), BF),
            pltpu.VMEM((STREAMS, 3, 4, 2, 3, HALF, LANES), BF),
            pltpu.VMEM((STREAMS, 3, 2, 3, HALF, LANES), BF),
            pltpu.VMEM((STREAMS, 3, 8, TILE, LANES), BF),
            pltpu.VMEM((STREAMS, 3, 7, TILE, LANES), BF),
            pltpu.VMEM((BATCH, PTS, LANES), F32),
            pltpu.VMEM((STREAMS, SLOTS + 1, TILE, LANES), F32),
            pltpu.VMEM((BATCH, PTS), F32),
            pltpu.SMEM((BATCH, LISTED), jnp.int32),
            pltpu.SMEM((2, 16), jnp.int32),
            dma((4 + STREAMS,)),
            dma((3, STREAMS)),
            dma((3, STREAMS)),
            dma((3, STREAMS)),
            dma((3, STREAMS, 4)),
            dma((3, STREAMS)),
            dma((3, STREAMS)),
            dma((STREAMS,)),
            dma((STREAMS,)),
            dma((STREAMS,)),
            dma((STREAMS,)),
        ],
        compiler_params=pltpu.CompilerParams(
            collective_id=0, has_side_effects=True, vmem_limit_bytes=60 * 1024 * 1024
        ),
    )(tiles, external, grid_values, kinetic, orbitals)


def solution(mesh):
    return jax.shard_map(
        body,
        mesh=mesh,
        in_specs=(
            P(("row", "col"), None, None),
            P(("row", "col"), None),
            P(("row", "col"), None),
            P("row", "col"),
            P(("row", "col"), None),
        ),
        out_specs=P(("row", "col"), None),
        check_vma=False,
    )
```
